32 devices in a mesh: row: 4 (over z), col: 8 (over y, x, core).
Axes of the slice: x: 2, y: 2, z: 4, core: 2. Of those that a mesh axis runs over, the one named last changes fastest.
Arguments:
- neighbor: int32 [32, 3072, 3072], P(None, 'col', 'row'), may hold values from 0 to 1, as said below
- true_coords: float32 [32, 3, 3072], P(None, None, ('row', 'col')), as said below
- pred_coords: float32 [32, 3, 3072], P(None, None, ('row', 'col')), as said below
- residue_mask: int32 [32, 3072], P(None, ('row', 'col')), may hold values from 0 to 1, as said below
- single: bfloat16 [32, 3072, 384], P(None, ('row', 'col'))
- ln_gain: float32 [384], replicated, may hold values from 0.1 to 1.9
- w_hidden: bfloat16 [384, 128], replicated, may hold values from -0.3125 to 0.3125
- b_hidden: float32 [128], replicated, may hold values from -3 to 3
- w_mid: bfloat16 [128, 128], replicated, may hold values from -0.5 to 0.5
- b_mid: float32 [128], replicated, may hold values from -3 to 3
- w_logits: bfloat16 [128, 50], replicated, may hold values from -1.5 to 1.5
- b_logits: float32 [50], replicated, may hold values from -4 to 4
Outputs:
- lddt_score: float32 [32, 3072], P(None, ('row', 'col'))
- residue_loss: float32 [32, 3072], P(None, ('row', 'col'))
- total_loss: float32 [], replicated
The draws below stay inside these ranges and needn't reach their ends.
Inputs may be any that keep to these rules, and one draw needn't show every extreme that they name: `neighbor`: 0 or 1; 0 where j == i; 1 wherever 0 < |i - j| <= 8. `residue_mask`: per structure, 1 on a leading run of 1536 or more residues and 0 after it. `true_coords`: positions in angstroms. `pred_coords`: positions in angstroms.
All inputs are finite; a program needn't handle non-finite values.
Results may differ from the reference program's by a relative error of at most 0.00098.
Values sent between devices are 32-bit elements; how exact they have to be, the bound alone decides.
A program may use at most 128 MiB of HBM per device.

```python
import math
import jax
import jax.numpy as jnp
from jax import lax

L = 3072
BATCH = 32
C_S = 384
HEAD_WIDTH = 128
BINS = 50


def chain_pair(key):
    base = jax.random.fold_in(key, 7)
    k_step, k_scale, k_noise = jax.random.split(base, 3)
    steps = jax.random.normal(k_step, (BATCH, 3, L), jnp.float32) * 2.2
    truth = jnp.cumsum(steps, axis=2)
    scale = jnp.exp(jax.random.uniform(k_scale, (BATCH, 1, L), jnp.float32, math.log(0.3), math.log(6.0)))
    noise = jax.random.normal(k_noise, (BATCH, 3, L), jnp.float32)
    return (truth, truth + scale * noise)


def draw_true_coords(key, part):
    return chain_pair(key)[0]


def draw_pred_coords(key, part):
    return chain_pair(key)[1]


def draw_neighbor(key, part):
    base = jax.random.fold_in(key, 13)
    rows_index = jnp.arange(L)[:, None]
    cols_index = jnp.arange(L)[None, :]
    apart = jnp.abs(rows_index - cols_index)
    banded = (apart <= 8) & (apart > 0)
    chosen = jax.random.randint(base, (BATCH, L, L), 0, 48) == 0
    linked = (banded[None] | chosen) & (apart > 0)[None]
    return jnp.where(linked, 1, 0).astype(jnp.int32)


def draw_residue_mask(key, part):
    base = jax.random.fold_in(key, 17)
    lengths = jax.random.randint(base, (BATCH, 1), L // 2, L + 1)
    positions = jnp.arange(L)[None, :]
    return jnp.where(positions < lengths, 1, 0).astype(jnp.int32)


def draw_single(key, part):
    base = jax.random.fold_in(key, 3)
    k_value = jax.random.fold_in(base, 0)
    values = jax.random.normal(k_value, (BATCH, L, C_S), jnp.float32)
    return values.astype(jnp.bfloat16)


def normal_values(own_key, extent, width, most, dtype=jnp.bfloat16):
    drawn = width * jax.random.normal(own_key, extent, jnp.float32)
    return jnp.clip(drawn, min=-most, max=most).astype(dtype)


def setup_inputs(seed: int = 0) -> dict:
    arg_keys = jax.random.split(jax.random.key(seed), 13)
    return {
        "neighbor": draw_neighbor(jax.random.fold_in(arg_keys[12], 71), 0),
        "true_coords": draw_true_coords(jax.random.fold_in(arg_keys[12], 71), 0),
        "pred_coords": draw_pred_coords(jax.random.fold_in(arg_keys[12], 71), 0),
        "residue_mask": draw_residue_mask(jax.random.fold_in(arg_keys[12], 71), 0),
        "single": draw_single(jax.random.fold_in(arg_keys[12], 71), 0),
        "ln_gain": jnp.clip(1.0 + 0.18 * jax.random.normal(arg_keys[5], (C_S,), jnp.float32), 0.1, 1.9),
        "w_hidden": normal_values(arg_keys[6], (C_S, HEAD_WIDTH), C_S ** -0.5, 0.3125),
        "b_hidden": normal_values(arg_keys[7], (HEAD_WIDTH,), 0.5, 3.0, jnp.float32),
        "w_mid": normal_values(arg_keys[8], (HEAD_WIDTH, HEAD_WIDTH), HEAD_WIDTH ** -0.5, 0.5),
        "b_mid": normal_values(arg_keys[9], (HEAD_WIDTH,), 0.5, 3.0, jnp.float32),
        "w_logits": normal_values(arg_keys[10], (HEAD_WIDTH, BINS), 0.25, 1.5),
        "b_logits": normal_values(arg_keys[11], (BINS,), 1.0, 4.0, jnp.float32),
    }


THRESHOLDS = (0.5, 1.0, 2.0, 4.0)

def pair_dist(near, far):
    total = (near[0][:, None] - far[0][None, :]) ** 2
    total = total + (near[1][:, None] - far[1][None, :]) ** 2
    total = total + (near[2][:, None] - far[2][None, :]) ** 2
    return jnp.sqrt(total + 1e-10)

def soft_preserved(true_dist, pred_dist):
    mismatch = jnp.abs(pred_dist - true_dist)
    scores = jnp.zeros_like(mismatch)
    for threshold in THRESHOLDS:
        scores = scores + jax.nn.sigmoid(4.0 * (threshold - mismatch))
    return 0.25 * scores

def head_loss(lddt_value, single, ln_gain, w_hidden, b_hidden, w_mid, b_mid, w_logits, b_logits):
    features = single.astype(jnp.float32)
    average = lax.optimization_barrier(jnp.mean(features, axis=-1, keepdims=True))
    centred = features - average
    variance = lax.optimization_barrier(jnp.mean(centred * centred, axis=-1, keepdims=True))
    normed = (centred * lax.rsqrt(variance + 1e-05) * ln_gain).astype(jnp.bfloat16)
    first_hidden = jax.nn.relu(jnp.dot(normed, w_hidden, preferred_element_type=jnp.float32) + b_hidden).astype(jnp.bfloat16)
    second_hidden = jax.nn.relu(jnp.dot(first_hidden, w_mid, preferred_element_type=jnp.float32) + b_mid).astype(jnp.bfloat16)
    logits = jnp.dot(second_hidden, w_logits, preferred_element_type=jnp.float32) + b_logits
    log_total = jnp.log(lax.optimization_barrier(jnp.sum(jnp.exp(logits), axis=-1)))
    bins = logits.shape[-1]
    centers = (jnp.arange(bins).astype(jnp.float32) + 0.5) / bins
    closeness = jnp.exp(-(lddt_value[..., None] - centers) ** 2 * (bins * bins * 0.5))
    target = closeness / lax.optimization_barrier(jnp.sum(closeness, axis=-1, keepdims=True))
    return log_total - lax.optimization_barrier(jnp.sum(target * logits, axis=-1))

def reference(neighbor, true_coords, pred_coords, residue_mask, single, ln_gain, w_hidden, b_hidden, w_mid, b_mid, w_logits, b_logits):
    valid = residue_mask.astype(jnp.float32)

    def per_structure(items):
        contacts, truth, guess, keep = items
        scores = soft_preserved(pair_dist(truth, truth), pair_dist(guess, guess))
        weights = contacts.astype(jnp.float32) * keep[None, :] * keep[:, None]
        return (lax.optimization_barrier(jnp.sum(weights * scores, axis=0)), lax.optimization_barrier(jnp.sum(weights, axis=0)))
    preserved, neighbors = lax.map(per_structure, (neighbor, true_coords, pred_coords, valid))
    lddt_score = preserved / jnp.maximum(neighbors, 1.0)
    residue_loss = valid * head_loss(lddt_score, single, ln_gain, w_hidden, b_hidden, w_mid, b_mid, w_logits, b_logits)
    total_loss = jnp.sum(residue_loss) / jnp.sum(valid)
    return (lddt_score, residue_loss, total_loss)
```

```python
import functools

import jax
import jax.numpy as jnp
from jax import lax
from jax.experimental import pallas as pl
from jax.experimental.pallas import tpu as pltpu
from jax.sharding import PartitionSpec as P

THRESHOLDS = (0.5, 1.0, 2.0, 4.0)
EPS = 1e-10
MESH = pl.DeviceIdType.MESH
CHUNK = 4
WIDTH = 256
F32 = jnp.float32
BF16 = jnp.bfloat16


def split3(x):
    first = x.astype(BF16).astype(F32)
    rest = x - first
    second = rest.astype(BF16).astype(F32)
    return first, second, rest - second


def with_norms(x, row):
    square = x * x
    true_norm = square[0:1] + square[1:2] + square[2:3]
    pred_norm = square[3:4] + square[4:5] + square[5:6]
    mixed = jnp.where(row < 6, x, jnp.where(row == 6, true_norm, pred_norm))
    return mixed, true_norm, pred_norm


def build_sides(rows, cols, left_t, left_p, right):
    keep = cols[6:7]
    center = jnp.sum(cols * keep, axis=1, keepdims=True) / jnp.maximum(jnp.sum(keep, axis=1, keepdims=True), 1.0)
    row_r = lax.broadcasted_iota(jnp.int32, rows.shape, 0)
    row_c = lax.broadcasted_iota(jnp.int32, cols.shape, 0)
    far, _, _ = with_norms((rows - center) * 2.0, row_r)
    near = (cols - center) * 2.0
    _, near_t, near_p = with_norms(near, row_c)
    f1, f2, f3 = split3(far)
    ones = jnp.ones_like(far)
    right[...] = jnp.concatenate([f1, f1, f1, f2, f2, f3, ones, jnp.zeros_like(far)], axis=0).astype(BF16)
    n1, n2, n3 = split3(near)
    zeros = jnp.zeros_like(near)
    for ref, low, norm_row, norm in ((left_t, 0, 6, near_t), (left_p, 3, 7, near_p)):
        inside = (row_c >= low) & (row_c < low + 3)
        l1 = jnp.where(inside, -2.0 * n1, jnp.where(row_c == norm_row, 1.0, 0.0))
        l2 = jnp.where(inside, -2.0 * n2, 0.0)
        l3 = jnp.where(inside, -2.0 * n3, 0.0)
        m1, m2, m3 = split3(norm)
        tail = jnp.where(
            row_c == 0, m1, jnp.where(row_c == 1, m2, jnp.where(row_c == 2, m3, jnp.where(row_c == 3, 4.0 * EPS, 0.0)))
        )
        side = jnp.concatenate([l1, l2, l3, l1, l2, l1, tail, zeros], axis=0)
        ref[...] = jnp.transpose(side).astype(BF16)


def build_keep(cols, keep):
    count = jnp.sum(cols[6:7], axis=1, keepdims=True)
    index = lax.broadcasted_iota(jnp.int32, keep.shape, 0).astype(F32)
    keep[...] = jnp.where(index < count, 1.0, 0.0).astype(BF16)


def distances(left_t, left_p, right, d_true, d_pred, q):
    side = right[:, q * WIDTH : (q + 1) * WIDTH]
    d_true[q] = jnp.dot(left_t[...], side, preferred_element_type=F32)
    d_pred[q] = jnp.dot(left_p[...], side, preferred_element_type=F32)


def gaps(d_true, d_pred, floor, gap, q, j, h):
    span, lanes = slice(j, j + 16), slice(h * 128, h * 128 + 128)
    t2 = jnp.maximum(d_true[q, span, lanes], floor)
    p2 = jnp.maximum(d_pred[q, span, lanes], floor)
    gap[q, span, lanes] = jnp.abs(p2 * lax.rsqrt(p2) - t2 * lax.rsqrt(t2))


def scores(gap, neighbor_ref, keep, q, j, h, sums):
    span, lanes = slice(j, j + 16), slice(h * 128, h * 128 + 128)
    total, count = sums
    g = gap[q, span, lanes]
    at = slice(q * WIDTH + h * 128, q * WIDTH + h * 128 + 128)
    linked = neighbor_ref[0, span, at].astype(jnp.int16) != 0
    w = jnp.where(linked, keep[span, :], jnp.zeros((16, 128), BF16)).astype(F32)
    x2 = (2.0 * THRESHOLDS[1] - g).astype(BF16)
    for x in (
        (2.0 * THRESHOLDS[3] - g).astype(BF16),
        (2.0 * THRESHOLDS[2] - g).astype(BF16),
        x2,
        x2 - BF16(2.0 * (THRESHOLDS[1] - THRESHOLDS[0])),
    ):
        term = jnp.tanh(x).astype(F32) * w
        total = term if total is None else total + term
    one = w * w
    count = one if count is None else count + one
    return total, count


def head(b, single, gain, wh, bh, wm, bm, wl, bl, logits_ref, total_ref):
    features = single[b].astype(F32)
    average = jnp.mean(features, axis=-1, keepdims=True)
    centred = features - average
    variance = jnp.mean(centred * centred, axis=-1, keepdims=True)
    normed = (centred * lax.rsqrt(variance + 1e-05) * gain).astype(BF16)
    first = jnp.maximum(jnp.dot(normed, wh[...], preferred_element_type=F32) + bh[...], 0.0).astype(BF16)
    second = jnp.maximum(jnp.dot(first, wm[...], preferred_element_type=F32) + bm[...], 0.0).astype(BF16)
    logits = lax.dot_general(wl[...], second, (((1,), (1,)), ((), ())), preferred_element_type=F32) + bl
    logits_ref[b] = logits
    total_ref[pl.ds(b, 1), :] = jnp.log(jnp.sum(jnp.exp(logits), axis=0, keepdims=True))


def kernel(
    R, C,
    true_ref, pred_ref, mask_ref, neighbor_ref, single_ref, gain_ref, wh_ref, bh_ref, wm_ref, bm_ref, wl_ref, bl_ref,
    lddt_ref, loss_ref, mean_ref,
    x_ref, rows_ref, cols_ref, single_v, logits_ref, total_ref,
    left_t, left_p, right, keep, floor_ref, d_true, d_pred, gap, acc,
    parts, landed, tile, tiles,
    single_sem, send_sem, recv_sem, csend_sem, crecv_sem, psend_sem, precv_sem, tsend_sem, trecv_sem,
):
    b = pl.program_id(0)
    batch = pl.num_programs(0)
    count_b = x_ref.shape[0]
    own_len = mask_ref.shape[1]
    rows_len = C * own_len
    cols_len = R * own_len
    chunks = count_b // CHUNK
    r = lax.axis_index("row")
    c = lax.axis_index("col")
    g = r * C + c
    to_col = g // R
    slot = g % R
    own = to_col == c

    def part(ref, n):
        return ref.at[pl.ds(n * CHUNK, CHUNK)]

    def row_copy(k, n):
        return pltpu.make_async_remote_copy(
            src_ref=part(x_ref, n),
            dst_ref=part(rows_ref.at[c], n),
            send_sem=send_sem.at[k, n],
            recv_sem=recv_sem.at[k, n],
            device_id=(r, (c + k) % C),
            device_id_type=MESH,
        )

    def col_copy(k, n):
        return pltpu.make_async_remote_copy(
            src_ref=part(x_ref, n),
            dst_ref=part(cols_ref.at[slot], n),
            send_sem=csend_sem.at[k, n],
            recv_sem=crecv_sem.at[slot, n],
            device_id=((r + k) % R, to_col),
            device_id_type=MESH,
        )

    def col_arrival(s, n):
        return pltpu.make_async_remote_copy(
            src_ref=part(x_ref, n),
            dst_ref=part(cols_ref.at[s], n),
            send_sem=csend_sem.at[0, n],
            recv_sem=crecv_sem.at[s, n],
            device_id=(r, to_col),
            device_id_type=MESH,
        )

    def arrive(n):
        for k in range(1, C):
            row_copy(k, n).wait_recv()
        for s in range(R):

            @pl.when(R * c + s != g)
            def _():
                col_arrival(s, n).wait_recv()

    def all_rows(i):
        return jnp.concatenate([rows_ref[s, i] for s in range(C)], axis=1)

    def all_cols(i):
        return jnp.concatenate([cols_ref[s, i] for s in range(R)], axis=1)

    @pl.when(b == 0)
    def _():
        fetch = pltpu.make_async_copy(single_ref, single_v, single_sem)
        fetch.start()
        barrier = pltpu.get_barrier_semaphore()
        for k in range(1, R * C):
            other = (g + k) % (R * C)
            pl.semaphore_signal(barrier, inc=1, device_id=(other // C, other % C), device_id_type=MESH)
        for k in range(3):
            x_ref[:, k, :] = true_ref[k]
            x_ref[:, 3 + k, :] = pred_ref[k]
        x_ref[:, 6, :] = mask_ref[...].astype(F32)
        x_ref[:, 7, :] = jnp.zeros(mask_ref.shape, F32)
        floor_ref[...] = jnp.full(floor_ref.shape, 4.0 * EPS, F32)
        pl.semaphore_wait(barrier, R * C - 1)

        def send(n, carry):
            for k in range(1, R):
                col_copy(k, n).start()

            @pl.when(jnp.logical_not(own))
            def _():
                col_copy(0, n).start()

            for k in range(1, C):
                row_copy(k, n).start()
            return carry

        lax.fori_loop(0, chunks, send, 0)
        rows_ref[c] = x_ref[...]

        @pl.when(own)
        def _():
            cols_ref[slot] = x_ref[...]

        bins = wl_ref.shape[0]
        eye = lax.broadcasted_iota(jnp.int32, (bins, bins), 0) == lax.broadcasted_iota(jnp.int32, (bins, bins), 1)
        bl = jnp.sum(jnp.where(eye, bl_ref[...], 0.0), axis=1, keepdims=True)
        gain = gain_ref[...]
        fetch.wait()

        def heads(n, carry):
            for k in range(CHUNK):
                head(
                    n * CHUNK + k, single_v, gain, wh_ref, bh_ref, wm_ref, bm_ref, wl_ref, bl, logits_ref, total_ref
                )
            return carry

        lax.fori_loop(0, chunks, heads, 0)
        arrive(0)
        for i in range(2):
            build_sides(all_rows(i), all_cols(i), left_t, left_p, right)
            for q in range(rows_len // WIDTH):
                distances(left_t, left_p, right, d_true, d_pred, q)
                if i == 0:
                    for j in range(0, cols_len, 16):
                        for h in range(WIDTH // 128):
                            gaps(d_true, d_pred, floor_ref[...], gap, q, j, h)
        build_sides(all_rows(2), all_cols(2), left_t, left_p, right)
        build_keep(all_cols(0), keep)

    ahead = b + 3

    @pl.when((ahead % CHUNK == 0) & (ahead < batch))
    def _():
        arrive(ahead // CHUNK)

    floor = floor_ref[...]
    for q in range(rows_len // WIDTH):
        sums = [(None, None)] * (WIDTH // 128)
        for j in range(0, cols_len, 16):
            for h in range(WIDTH // 128):
                sums[h] = scores(gap, neighbor_ref, keep, q, j, h, sums[h])
                gaps(d_true, d_pred, floor, gap, q, j, h)
        distances(left_t, left_p, right, d_true, d_pred, q)
        for h in range(WIDTH // 128):
            at = slice(q * WIDTH + h * 128, q * WIDTH + h * 128 + 128)
            count = jnp.sum(sums[h][1], axis=0, keepdims=True)
            acc[b, 1:2, at] = count
            acc[b, 0:1, at] = 0.5 * count + 0.125 * jnp.sum(sums[h][0], axis=0, keepdims=True)
    later = jnp.minimum(ahead, batch - 1)
    build_sides(all_rows(later), all_cols(later), left_t, left_p, right)
    build_keep(all_cols(jnp.minimum(b + 1, batch - 1)), keep)

    @pl.when(b == batch - 1)
    def _():
        for s in range(C):
            lanes = slice(s * own_len, (s + 1) * own_len)
            parts[s, 0:count_b, :] = acc[:, 0, lanes]
            parts[s, count_b:, :] = acc[:, 1, lanes]
        copies = []
        for k in range(1, C):
            peer = (c + k) % C
            copy = pltpu.make_async_remote_copy(
                src_ref=parts.at[peer],
                dst_ref=landed.at[k],
                send_sem=psend_sem.at[k],
                recv_sem=precv_sem.at[k],
                device_id=(r, peer),
                device_id_type=MESH,
            )
            copy.start()
            copies.append(copy)
        sums = parts[c]

        def sent(n, carry):
            for k in range(1, R):
                col_copy(k, n).wait_send()

            @pl.when(jnp.logical_not(own))
            def _():
                col_copy(0, n).wait_send()

            for k in range(1, C):
                row_copy(k, n).wait_send()
            return carry

        lax.fori_loop(0, chunks, sent, 0)
        for copy in copies:
            copy.wait()
        for k in range(1, C):
            sums = sums + landed[k]
        valid = x_ref[:, 6, :]
        lddt = valid * sums[0:count_b] / jnp.maximum(valid * sums[count_b:], 1.0)
        lddt_ref[...] = lddt
        bins = logits_ref.shape[1]
        logits = logits_ref[...]
        centers = (lax.broadcasted_iota(jnp.int32, logits.shape, 1).astype(F32) + 0.5) / bins
        apart = lddt[:, None, :] - centers
        closeness = jnp.exp(-(apart * apart) * (bins * bins * 0.5))
        expected = jnp.sum(closeness * logits, axis=1) / jnp.sum(closeness, axis=1)
        loss = valid * (total_ref[...] - expected)
        tile[...] = jnp.zeros_like(tile)
        tile[0:1, 0:own_len] = jnp.sum(loss, axis=0, keepdims=True)
        tile[1:2, 0:own_len] = jnp.sum(valid, axis=0, keepdims=True)
        loss_ref[...] = loss
        copies = []
        for k in range(1, R * C):
            other = (g + k) % (R * C)
            copy = pltpu.make_async_remote_copy(
                src_ref=tile,
                dst_ref=tiles.at[g],
                send_sem=tsend_sem.at[k],
                recv_sem=trecv_sem.at[k],
                device_id=(other // C, other % C),
                device_id_type=MESH,
            )
            copy.start()
            copies.append(copy)
        tiles[g] = tile[...]
        for copy in copies:
            copy.wait()
        final = tiles[0]
        for k in range(1, R * C):
            final = final + tiles[k]
        both = jnp.sum(final, axis=1, keepdims=True)
        mean_ref[...] = jnp.broadcast_to(both[0:1] / both[1:2], mean_ref.shape)


def local(
    R, C,
    neighbor,
    true_coords,
    pred_coords,
    residue_mask,
    single,
    ln_gain,
    w_hidden,
    b_hidden,
    w_mid,
    b_mid,
    w_logits,
    b_logits,
):
    batch, own_len = residue_mask.shape
    cols_len, rows_len = neighbor.shape[1:]
    bins = w_logits.shape[1]
    whole = pl.BlockSpec(memory_space=pltpu.VMEM)
    chunks = batch // CHUNK
    tiles = rows_len // WIDTH
    dma = pltpu.SemaphoreType.DMA
    lddt, loss, mean = pl.pallas_call(
        functools.partial(kernel, R, C),
        grid=(batch,),
        in_specs=[
            whole,
            whole,
            whole,
            pl.BlockSpec((1, cols_len, rows_len), lambda i: (i, 0, 0)),
            pl.BlockSpec(memory_space=pl.ANY),
        ]
        + [whole] * 7,
        out_specs=[whole] * 3,
        out_shape=[
            jax.ShapeDtypeStruct((batch, own_len), F32),
            jax.ShapeDtypeStruct((batch, own_len), F32),
            jax.ShapeDtypeStruct((8, 128), F32),
        ],
        scratch_shapes=[
            pltpu.VMEM((batch, 8, own_len), F32),
            pltpu.VMEM((C, batch, 8, own_len), F32),
            pltpu.VMEM((R, batch, 8, own_len), F32),
            pltpu.VMEM(single.shape, single.dtype),
            pltpu.VMEM((batch, bins, own_len), F32),
            pltpu.VMEM((batch, own_len), F32),
            pltpu.VMEM((cols_len, 64), BF16),
            pltpu.VMEM((cols_len, 64), BF16),
            pltpu.VMEM((64, rows_len), BF16),
            pltpu.VMEM((cols_len, 128), BF16),
            pltpu.VMEM((16, 128), F32),
            pltpu.VMEM((tiles, cols_len, WIDTH), F32),
            pltpu.VMEM((tiles, cols_len, WIDTH), F32),
            pltpu.VMEM((tiles, cols_len, WIDTH), F32),
            pltpu.VMEM((batch, 2, rows_len), F32),
            pltpu.VMEM((C, 2 * batch, own_len), F32),
            pltpu.VMEM((C, 2 * batch, own_len), F32),
            pltpu.VMEM((8, 128), F32),
            pltpu.VMEM((R * C, 8, 128), F32),
            dma,
            dma((C, chunks)),
            dma((C, chunks)),
            dma((R, chunks)),
            dma((R, chunks)),
            dma((C,)),
            dma((C,)),
            dma((R * C,)),
            dma((R * C,)),
        ],
        compiler_params=pltpu.CompilerParams(
            dimension_semantics=("arbitrary",), collective_id=0, has_side_effects=True
        ),
        name="lddt",
    )(
        jnp.transpose(true_coords, (1, 0, 2)),
        jnp.transpose(pred_coords, (1, 0, 2)),
        residue_mask,
        neighbor,
        single,
        ln_gain[None, :],
        w_hidden,
        b_hidden[None, :],
        w_mid,
        b_mid[None, :],
        w_logits.T,
        b_logits[None, :],
    )
    return (lddt, loss, mean[0, 0])


def solution(mesh):
    R = mesh.shape["row"]
    C = mesh.shape["col"]
    both = P(None, ("row", "col"))
    placed = (
        P(None, "col", "row"),
        P(None, None, ("row", "col")),
        P(None, None, ("row", "col")),
        both,
        P(None, ("row", "col"), None),
        P(),
        P(),
        P(),
        P(),
        P(),
        P(),
        P(),
    )
    return jax.shard_map(
        functools.partial(local, R, C),
        mesh=mesh,
        in_specs=placed,
        out_specs=(both, both, P()),
        check_vma=False,
    )
```
